32 devices in a mesh: seq: 8 (over z, y), head: 4 (over x, core).
Axes of the slice: x: 2, y: 2, z: 4, core: 2. Of those that a mesh axis runs over, the one named last changes fastest.
Arguments:
- query: bfloat16 [512, 2048], P('seq', 'head'), may hold values from -16 to 16
- key_states: bfloat16 [512, 2048], P('seq', 'head'), may hold values from -16 to 16
- value_states: bfloat16 [512, 2048], P('seq', 'head'), may hold values from -6 to 6
- doc_ids: int32 [512], P('seq'), may hold values from 0 to 3, never falling along the last dimension, each value on 1 to 256 neighbouring positions
- out_weight: bfloat16 [2048, 4096], P('head', 'seq'), may hold values from -0.1875 to 0.1875
- residual: bfloat16 [512, 4096], P('seq', 'head'), may hold values from -6 to 6
Outputs:
- mixed: bfloat16 [512, 4096], P('seq', 'head')
The draws below stay inside these ranges and needn't reach their ends.
Inputs may be any that keep to these rules, and one draw needn't show every extreme that they name: doc_ids never fall along the sequence; every document has 1 to 256 positions, and one has exactly 256.
All inputs are finite; a program needn't handle non-finite values.
Results may differ from the reference program's by a relative error of at most 0.0055.
Values may be sent and summed in bfloat16 or wider, within the bound.
A program may use at most 64 MiB of HBM per device.

```python
import math
import jax
import jax.numpy as jnp
import numpy as np
from jax import lax

D = 4096
HEAD_DIM = 128
HEADS = 16
DOCS = 4
SEQ = 512
DOC_MOST = 256


def drawn_pair(key):
    base = jax.random.fold_in(key, 7)
    first, second = jax.random.split(base, 2)
    width = HEADS * HEAD_DIM
    queries = 1.7 * jnp.clip(jax.random.normal(first, (SEQ, width), jnp.float32), -4.5, 4.5)
    keys = 1.7 * jnp.clip(jax.random.normal(second, (SEQ, width), jnp.float32), -4.5, 4.5)
    return (queries, keys)


def draw_query(key, part):
    return drawn_pair(key)[0].astype(jnp.bfloat16)


def draw_key_states(key, part):
    return drawn_pair(key)[1].astype(jnp.bfloat16)


def spiked(drawn, rng, source, target, blocks, factor):
    owner, partner = [(jnp.arange(drawn.shape[position]) // (drawn.shape[position] // blocks)).reshape([-1 if axis == position else 1 for axis in range(drawn.ndim)]) for position in (source, target)]
    chosen = jax.random.permutation(rng, blocks)[partner]
    strong = (owner == chosen) | (owner == (partner + blocks // 2) % blocks)
    return jnp.where(strong, factor * drawn, drawn)


def block_scale(own_key, dims, cuts, least, largest):
    def one(dim, parts):
        heights = jax.random.uniform(jax.random.fold_in(jax.random.fold_in(own_key, 6), dim), (parts,), jnp.float32, least / len(cuts), largest / len(cuts))
        return jnp.repeat(jnp.exp(heights), dims[dim] // parts).reshape((-1,) + (1,) * (len(dims) - dim - 1))

    level = one(*cuts[0])
    for cut in cuts[1:]:
        level = level * one(*cut)
    return level


def split_up(count, total, most, skew):
    portions = [(1 << 20) // math.isqrt(standing ** skew) + 1 for standing in range(2, count + 1)]
    spare, given = total - most - (count - 1), [1] * (count - 1)
    while spare > 0:
        movable = [i for i in range(count - 1) if given[i] < most]
        pool, left = sum([portions[i] for i in movable]), spare
        for i in movable:
            addition = min(most - given[i], max(1, left * portions[i] // pool), spare)
            given[i] = given[i] + addition
            spare = spare - addition
    return np.array([most] + given)


def ragged(key, count, total, limit, slope):
    if count == 2:
        one = jax.random.randint(key, (), max(1, total - limit), min(limit, total - 1) + 1)
        return jnp.stack([one, total - one])
    sizes = jnp.asarray(split_up(count, total, limit, slope), jnp.int32)
    twos = (count - 1) // 2
    giver, sink = sizes[1:1 + 2 * twos:2], sizes[2:2 + 2 * twos:2]
    room = jnp.minimum(giver - 1, limit - sink)
    moved = jax.random.randint(jax.random.fold_in(key, 1), (twos,), 0, 1 << 20) % (room + 1)
    sizes = sizes.at[1:1 + 2 * twos:2].set(giver - moved).at[2:2 + 2 * twos:2].set(sink + moved)
    return sizes[jax.random.permutation(jax.random.fold_in(key, 2), count)]


def noise(own_key, shape, deviation, limit, shards=(), held_as=jnp.bfloat16):
    drawn = jax.random.normal(own_key, shape, jnp.float32) * deviation
    if len(shards) > 0:
        drawn = block_scale(own_key, shape, shards, -0.22, 0.18) * drawn
    return jnp.clip(drawn, min=-limit, max=limit).astype(held_as)


def heavy_noise(rng, extent, spread, reach, cuts, heavy, kind=jnp.bfloat16):
    result = spread * jax.random.normal(rng, extent, jnp.float32)
    if cuts:
        result = result * block_scale(rng, extent, cuts, -0.22, 0.18)
    return jnp.clip(spiked(result, jax.random.fold_in(rng, 3), *heavy), -reach, reach).astype(kind)


def setup_inputs(seed: int = 0) -> dict:
    splits = jax.random.split(jax.random.key(seed), 7)
    query = draw_query(jax.random.fold_in(splits[6], 71), 0)
    key_states = draw_key_states(jax.random.fold_in(splits[6], 71), 0)
    value_states = noise(splits[2], (SEQ, HEADS * HEAD_DIM), 1.0, 6.0, ((0, 8), (1, 4)))
    doc_ids = jnp.searchsorted(jnp.cumsum(ragged(splits[3], DOCS, SEQ, DOC_MOST, 1)), jnp.arange(SEQ), side="right").astype(jnp.int32)
    out_weight = heavy_noise(splits[4], (HEADS * HEAD_DIM, D), (HEADS * HEAD_DIM) ** -0.5, 0.1875, ((0, 4), (1, 8)), (0, 1, 8, 2.0))
    residual = noise(splits[5], (SEQ, D), 1.0, 6.0, ((0, 8), (1, 4)))
    return {"query": query, "key_states": key_states, "value_states": value_states, "doc_ids": doc_ids, "out_weight": out_weight, "residual": residual}


masked_score = -1.0e30


def reference(query, key_states, value_states, doc_ids, out_weight, residual):
    positions = jnp.arange(SEQ, dtype=jnp.int32)
    allowed = (positions[None, :] <= positions[:, None]) & (doc_ids[None, :] == doc_ids[:, None])
    query_heads = query.reshape(SEQ, HEADS, HEAD_DIM).transpose(1, 0, 2)
    key_heads = key_states.reshape(SEQ, HEADS, HEAD_DIM).transpose(1, 0, 2)
    value_heads = value_states.reshape(SEQ, HEADS, HEAD_DIM).transpose(1, 0, 2)

    def one_head(operands):
        queries, keys, values = operands
        scores = jnp.dot(queries, keys.T, preferred_element_type=jnp.float32) * (HEAD_DIM ** -0.5)
        scores = jnp.where(allowed, scores, masked_score)
        row_max = jnp.max(scores, axis=1, keepdims=True)
        weights = jnp.where(allowed, jnp.exp(scores - row_max), 0.0)
        row_sum = jnp.sum(weights, axis=1, keepdims=True)
        attended = jnp.dot(weights.astype(jnp.bfloat16), values, preferred_element_type=jnp.float32) / row_sum
        return attended.astype(jnp.bfloat16)

    per_head = lax.map(one_head, (query_heads, key_heads, value_heads))
    attended = per_head.transpose(1, 0, 2).reshape(SEQ, HEADS * HEAD_DIM)
    mixed = residual.astype(jnp.float32) + jnp.dot(attended, out_weight, preferred_element_type=jnp.float32)
    return mixed.astype(jnp.bfloat16)
```

```python
import functools

import jax
import jax.numpy as jnp
from jax import lax
from jax.experimental import pallas as pl
from jax.experimental.pallas import tpu as pltpu
from jax.sharding import PartitionSpec as P

HEAD_DIM = 128


masked_score = -1e30


def to_heads(block):
    return block.reshape(block.shape[0], block.shape[1] // HEAD_DIM, HEAD_DIM)


def attend_block(state, queries, query_pos, query_docs, keys, values, key_pos, key_docs):
    run_max, run_sum, run_acc = state
    scores = jnp.einsum(
        "qhd,khd->hqk", queries, keys, preferred_element_type=jnp.float32
    ) * HEAD_DIM ** (-0.5)
    allowed = (key_pos[None, :] <= query_pos[:, None]) & (key_docs[None, :] == query_docs[:, None])
    scores = jnp.where(allowed[None], scores, masked_score)
    new_max = jnp.maximum(run_max, jnp.max(scores, axis=-1))
    weights = jnp.where(allowed[None], jnp.exp(scores - new_max[..., None]), 0.0)
    run_sum = jnp.sum(weights, axis=-1)
    run_acc = jnp.einsum(
        "hqk,khd->hqd", weights.astype(jnp.bfloat16), values, preferred_element_type=jnp.float32
    )
    return (new_max, run_sum, run_acc)


def shards(query, key_states, value_states, doc_ids, out_weight, residual):
    tok_rows = query.shape[0]
    heads = query.shape[1] // HEAD_DIM
    shard_index = lax.axis_index("seq")
    first_pos = shard_index * tok_rows
    groups = [(query, first_pos + jnp.arange(tok_rows, dtype=jnp.int32), doc_ids)]
    prepared = [(to_heads(block), block_pos, block_docs) for block, block_pos, block_docs in groups]
    initial = tuple(
        (
            (
                jnp.full((heads, block_pos.shape[0]), masked_score, jnp.float32),
                jnp.zeros((heads, block_pos.shape[0]), jnp.float32),
                jnp.zeros((heads, block_pos.shape[0], HEAD_DIM), jnp.float32),
            )
            for block, block_pos, block_docs in groups
        )
    )
    first_row = jnp.int32(0)
    keys = lax.all_gather(key_states, "seq", axis=0, tiled=True)
    values = lax.all_gather(value_states, "seq", axis=0, tiled=True)
    key_docs = lax.all_gather(doc_ids, "seq", axis=0, tiled=True)
    key_pos = jnp.arange(keys.shape[0], dtype=jnp.int32)
    key_heads = to_heads(keys)
    value_heads = to_heads(values)
    updated = []
    for member, state in zip(prepared, initial):
        queries, query_pos, query_docs = member

        def advance(inner, queries=queries, query_pos=query_pos, query_docs=query_docs):
            return attend_block(
                inner, queries, query_pos, query_docs, key_heads, value_heads, key_pos, key_docs
            )

        def unchanged(inner):
            return inner

        updated.append(lax.cond(first_row <= jnp.max(query_pos), advance, unchanged, state))
    finals = tuple(updated)
    outputs = []
    for run_max, run_sum, run_acc in finals:
        normed = run_acc / run_sum[..., None]
        outputs.append(
            jnp.transpose(normed, (1, 0, 2))
            .reshape(normed.shape[1], heads * HEAD_DIM)
            .astype(jnp.bfloat16)
        )
    attended = outputs[0]
    mapped = jnp.dot(
        attended,
        lax.all_gather(out_weight, "seq", axis=1, tiled=True),
        preferred_element_type=jnp.float32,
    )
    summed = lax.psum_scatter(mapped, "head", scatter_dimension=1, tiled=True)
    return (residual.astype(jnp.float32) + summed).astype(jnp.bfloat16)


MESH = pl.DeviceIdType.MESH


STEPS = 2


def attention(queries, keys, values, doc_row, row_pos):
    rows, keep = queries.shape[0], keys.shape[0]
    scores = lax.dot_general(
        queries, keys, (((1,), (1,)), ((), ())), preferred_element_type=jnp.float32
    ) * HEAD_DIM ** (-0.5)
    col_pos = lax.broadcasted_iota(jnp.int32, (rows, keep), 1)
    docs = jnp.broadcast_to(doc_row, (rows, keep))
    query_docs = jnp.sum(jnp.where(row_pos == col_pos, docs, 0), axis=1, keepdims=True)
    allowed = (col_pos <= row_pos) & (docs == query_docs)
    scores = jnp.where(allowed, scores, masked_score)
    row_max = jnp.max(scores, axis=1, keepdims=True)
    weights = jnp.where(allowed, jnp.exp(scores - row_max), 0.0)
    row_sum = jnp.sum(weights, axis=1, keepdims=True)
    product = jnp.dot(weights.astype(jnp.bfloat16), values, preferred_element_type=jnp.float32)
    return (product / row_sum).astype(jnp.bfloat16)


def fused_kernel(
    nz, q_ref, k_ref, v_ref, doc_ref, w_ref, res_ref, out_ref,
    qin, kin, vin, docin, qbuf, kbuf, vbuf, docbuf, att, wbuf, sendbuf, parts, resbuf,
    in_sem, q_send, q_recv, k_send, k_recv, v_send, v_recv, d_send, d_recv,
    z_send, z_recv, f_send, f_recv, p_send, p_recv, w_send, w_recv, res_sem, near,
):
    me = lax.axis_index("seq")
    head = lax.axis_index("head")
    rows = k_ref.shape[0]
    z, y = me // 2, me % 2
    x, core = head // 2, head % 2
    wrows = w_ref.shape[0]
    wcols = w_ref.shape[1]

    barrier = pltpu.get_barrier_semaphore()

    def greet(sem, to):
        pl.semaphore_signal(sem, inc=1, device_id=to, device_id_type=MESH)

    def beside(far, act):
        for side, step in enumerate((-far, far)):
            @pl.when((z + step >= 0) & (z + step < nz))
            def _(side=side, step=step):
                act(side, z + step)

    beside(1, lambda side, to: greet(barrier, (2 * to + y, head)))
    for dy in range(2):
        for dh in range(4):
            if dy or dh:
                greet(barrier, (2 * z + lax.rem(y + dy, 2), lax.rem(head + dh, 4)))

    def lanes(ref, index):
        return ref.at[:, pl.ds(pl.multiple_of(index * HEAD_DIM, HEAD_DIM), HEAD_DIM)]

    def block(ref, index):
        return ref.at[pl.ds(pl.multiple_of(index * rows, rows), rows), :]

    kinds = ((kin, kbuf, k_send, k_recv), (vin, vbuf, v_send, v_recv))
    staged = [
        pltpu.make_async_copy(src, dst, in_sem.at[index])
        for index, (src, dst) in enumerate(
            ((k_ref, kin), (v_ref, vin), (q_ref, qin), (doc_ref, docin))
        )
    ]
    for copy in staged:
        copy.start()
    for src, (_, dst, _, recv) in zip((k_ref, v_ref), kinds):
        pltpu.make_async_copy(lanes(src, z), block(dst, me), recv.at[me]).start()
    pltpu.make_async_copy(lanes(q_ref, z), block(qbuf, z), q_recv.at[z]).start()
    pltpu.make_async_copy(doc_ref, docbuf.at[me], d_recv.at[me]).start()
    res_copy = pltpu.make_async_copy(res_ref, resbuf, res_sem)
    res_copy.start()

    w_slot = wbuf.at[pl.ds(pl.multiple_of(core * wrows, wrows), wrows), :]

    @pl.when(core == y)
    def _():
        pltpu.make_async_copy(w_ref, w_slot, w_recv.at[core]).start()

    pl.semaphore_wait(
        barrier, 7 + (z > 0).astype(jnp.int32) + (z < nz - 1).astype(jnp.int32)
    )

    def relay(turn):
        beside(1, lambda side, to: greet(near.at[turn, 1 - side], (2 * to + y, head)))

    def relayed(turn):
        beside(1, lambda side, to: pl.semaphore_wait(near.at[turn, side], 1))

    def arrived(ref, sem):
        pltpu.make_async_copy(ref, ref, sem).wait()

    def remote(src, dst, send, recv, to):
        return pltpu.make_async_remote_copy(
            src_ref=src, dst_ref=dst, send_sem=send, recv_sem=recv,
            device_id=to, device_id_type=MESH,
        )

    def send_kv(kind, to):
        src, dst, send, recv = kind
        return remote(
            lanes(src, to // 2), block(dst, me), send.at[to], recv.at[me], (to, head)
        )

    def send_q(to):
        return remote(
            lanes(qin, to // 2), block(qbuf, z), q_send.at[to], q_recv.at[z], (to, head)
        )

    def send_doc(to):
        return remote(docin, docbuf.at[me], d_send.at[to], d_recv.at[me], (to, head))

    def own_column(to):
        return [send_doc(to), send_kv(kinds[0], to), send_q(to), send_kv(kinds[1], to)]

    def other_column(to):
        return [send_doc(to), send_kv(kinds[0], to), send_kv(kinds[1], to)]

    def exchange(far, column, copies, act):
        def each(side, to):
            for copy in copies(2 * to + column):
                act(copy)

        beside(far, each)

    def start(copy):
        copy.start()

    def sent(copy):
        copy.wait_send()

    relay(0)
    for copy in staged:
        copy.wait()

    across = 2 * z + 1 - y
    for copy in other_column(across):
        copy.start()
    w_across = remote(w_ref, w_slot, w_send.at[0], w_recv.at[core], (across, 2 * x + y))
    w_beside = remote(w_ref, w_slot, w_send.at[1], w_recv.at[core], (me, 2 * x + y))
    w_across.start()

    @pl.when(core != y)
    def _():
        w_beside.start()

    exchange(1, y, own_column, start)
    for far in range(1, nz):
        relayed(far - 1)
        if far < nz - 1:
            relay(far)
        exchange(far, 1 - y, other_column, start)
        if far < nz - 1:
            exchange(far + 1, y, own_column, start)

    deep = nz // STEPS
    part = deep * rows
    row_id = lax.broadcasted_iota(jnp.int32, (part, 1), 0)
    row_pos = row_id + y * rows
    for index in range(1, deep):
        row_pos = row_pos + jnp.where(row_id >= index * rows, rows, 0)

    def att_part(c, source, step):
        return att.at[c * nz + source, pl.ds(step * part, part), :]

    def att_copy(source, step, send, recv, to):
        ref = att_part(core, source, step)
        return remote(ref, ref, send, recv, to)

    def along(to, step):
        return att_copy(z, step, z_send.at[to, step], z_recv.at[z, step], (2 * to + y, head))

    def forward(source, step):
        return att_copy(
            source, step, f_send.at[source, step], f_recv.at[source, step],
            (me, 2 * x + 1 - core),
        )

    for step in range(STEPS):
        for source in range(deep * step, deep * (step + 1)):
            arrived(qbuf.at[pl.ds(source * rows, rows), :], q_recv.at[source])
        for source in range(2 * deep * step, 2 * deep * (step + 1)):
            arrived(docbuf.at[source], d_recv.at[source])
            for _, dst, _, recv in kinds:
                arrived(dst.at[pl.ds(source * rows, rows), :], recv.at[source])
        seen = 2 * deep * (step + 1)
        att[core * nz + z, pl.ds(step * part, part), :] = attention(
            qbuf[step * part:(step + 1) * part, :],
            kbuf[:seen * rows, :],
            vbuf[:seen * rows, :],
            jnp.concatenate([docbuf[source] for source in range(seen)], axis=1),
            row_pos + 2 * part * step,
        )
        for far in reversed(range(1, nz)):
            beside(far, lambda side, to, step=step: along(to, step).start())
        forward(z, step).start()

    slot = 2 * x + core

    def deliver(index, act, act_own=None):
        own = (me == 2 * index + y) & (head == z)
        src = sendbuf.at[pl.ds(index * rows, rows), :]

        if act_own:
            @pl.when(own)
            def _():
                act_own(pltpu.make_async_copy(src, parts.at[slot], p_recv.at[slot]))

        @pl.when(jnp.logical_not(own))
        def _():
            act(remote(
                src, parts.at[slot], p_send.at[index], p_recv.at[slot], (2 * index + y, z)
            ))

    for step in range(STEPS):
        for far in range(1, nz):
            def pass_on(side, source, step=step):
                arrived(att_part(core, source, step), z_recv.at[source, step])
                forward(source, step).start()

            beside(far, pass_on)
        for source in range(nz):
            arrived(att_part(1 - core, source, step), f_recv.at[source, step])
        if step == 0:
            for index in range(2):
                arrived(wbuf.at[pl.ds(index * wrows, wrows), :], w_recv.at[index])
        attended = jnp.concatenate(
            [att[index, step * part:(step + 1) * part, :] for index in range(2 * nz)], axis=1
        )
        sendbuf[step * part:(step + 1) * part, :] = jnp.dot(
            attended, wbuf[...], preferred_element_type=jnp.float32
        ).astype(jnp.bfloat16)
        for index in range(deep * step, deep * (step + 1)):
            deliver(index, start, start)

    res_copy.wait()
    for c in range(2):
        for p in range(2):
            arrived(parts.at[2 * p + c], p_recv.at[2 * p + c])
        cols = slice(c * wcols, (c + 1) * wcols)
        total = parts[c].astype(jnp.float32) + parts[2 + c].astype(jnp.float32)
        out_ref[:, cols] = (resbuf[:, cols].astype(jnp.float32) + total).astype(jnp.bfloat16)

    for copy in other_column(across):
        copy.wait_send()
    w_across.wait_send()

    @pl.when(core != y)
    def _():
        w_beside.wait_send()

    for far in range(1, nz):
        exchange(far, y, own_column, sent)
        exchange(far, 1 - y, other_column, sent)
        for step in range(STEPS):
            beside(far, lambda side, to, step=step: along(to, step).wait_send())
    for step in range(STEPS):
        for source in range(nz):
            forward(source, step).wait_send()
    for index in range(nz):
        deliver(index, sent)


def fused(n, query, key_states, value_states, doc_ids, out_weight, residual):
    rows, width = key_states.shape
    wrows, wcols = out_weight.shape
    seq, nz = n * rows, n // 2
    dma = pltpu.SemaphoreType.DMA
    any_ = pl.BlockSpec(memory_space=pl.ANY)
    bf16 = jnp.bfloat16
    return pl.pallas_call(
        functools.partial(fused_kernel, nz),
        out_shape=jax.ShapeDtypeStruct(residual.shape, residual.dtype),
        in_specs=[any_] * 6,
        out_specs=pl.BlockSpec(memory_space=pltpu.VMEM),
        scratch_shapes=[
            pltpu.VMEM((rows, width), bf16),
            pltpu.VMEM((rows, width), bf16),
            pltpu.VMEM((rows, width), bf16),
            pltpu.VMEM((1, rows), jnp.int32),
            pltpu.VMEM((seq // 2, HEAD_DIM), bf16),
            pltpu.VMEM((seq, HEAD_DIM), bf16),
            pltpu.VMEM((seq, HEAD_DIM), bf16),
            pltpu.VMEM((n, 1, rows), jnp.int32),
            pltpu.VMEM((n, seq // 2, HEAD_DIM), bf16),
            pltpu.VMEM((2 * wrows, wcols), bf16),
            pltpu.VMEM((seq // 2, wcols), bf16),
            pltpu.VMEM((4, rows, wcols), bf16),
            pltpu.VMEM(residual.shape, bf16),
            dma((4,)),
            dma((n,)), dma((nz,)),
            dma((n,)), dma((n,)),
            dma((n,)), dma((n,)),
            dma((n,)), dma((n,)),
            dma((nz, STEPS)), dma((nz, STEPS)),
            dma((nz, STEPS)), dma((nz, STEPS)),
            dma((nz,)), dma((4,)),
            dma((2,)), dma((2,)), dma,
            pltpu.SemaphoreType.REGULAR((nz - 1, 2)),
        ],
        compiler_params=pltpu.CompilerParams(collective_id=0, has_side_effects=True),
    )(query, key_states, value_states, doc_ids.reshape(1, rows), out_weight, residual)


def solution(mesh):
    placed = (
        P("seq", "head"),
        P("seq", "head"),
        P("seq", "head"),
        P("seq"),
        P("head", "seq"),
        P("seq", "head"),
    )
    n, nh = mesh.shape["seq"], mesh.shape["head"]

    def body(query, key_states, value_states, doc_ids, out_weight, residual):
        heads = query.shape[1] // HEAD_DIM
        fits = (
            n == 2 * heads
            and n == 2 * nh
            and nh == 4
            and out_weight.shape[1] % 256 == 0
            and query.shape[0] % 16 == 0
        )
        run = functools.partial(fused, n) if fits else shards
        return run(query, key_states, value_states, doc_ids, out_weight, residual)

    return jax.shard_map(
        body, mesh=mesh, in_specs=placed, out_specs=P("seq", "head"), check_vma=False
    )
```

```python
import functools

import jax
import jax.numpy as jnp
from jax import lax
from jax.experimental import pallas as pl
from jax.experimental.pallas import tpu as pltpu
from jax.sharding import PartitionSpec as P

HEAD_DIM = 128


masked_score = -1e30


def to_heads(block):
    return block.reshape(block.shape[0], block.shape[1] // HEAD_DIM, HEAD_DIM)


def attend_block(state, queries, query_pos, query_docs, keys, values, key_pos, key_docs):
    run_max, run_sum, run_acc = state
    scores = jnp.einsum(
        "qhd,khd->hqk", queries, keys, preferred_element_type=jnp.float32
    ) * HEAD_DIM ** (-0.5)
    allowed = (key_pos[None, :] <= query_pos[:, None]) & (key_docs[None, :] == query_docs[:, None])
    scores = jnp.where(allowed[None], scores, masked_score)
    new_max = jnp.maximum(run_max, jnp.max(scores, axis=-1))
    weights = jnp.where(allowed[None], jnp.exp(scores - new_max[..., None]), 0.0)
    run_sum = jnp.sum(weights, axis=-1)
    run_acc = jnp.einsum(
        "hqk,khd->hqd", weights.astype(jnp.bfloat16), values, preferred_element_type=jnp.float32
    )
    return (new_max, run_sum, run_acc)


def shards(query, key_states, value_states, doc_ids, out_weight, residual):
    tok_rows = query.shape[0]
    heads = query.shape[1] // HEAD_DIM
    shard_index = lax.axis_index("seq")
    first_pos = shard_index * tok_rows
    groups = [(query, first_pos + jnp.arange(tok_rows, dtype=jnp.int32), doc_ids)]
    prepared = [(to_heads(block), block_pos, block_docs) for block, block_pos, block_docs in groups]
    initial = tuple(
        (
            (
                jnp.full((heads, block_pos.shape[0]), masked_score, jnp.float32),
                jnp.zeros((heads, block_pos.shape[0]), jnp.float32),
                jnp.zeros((heads, block_pos.shape[0], HEAD_DIM), jnp.float32),
            )
            for block, block_pos, block_docs in groups
        )
    )
    first_row = jnp.int32(0)
    keys = lax.all_gather(key_states, "seq", axis=0, tiled=True)
    values = lax.all_gather(value_states, "seq", axis=0, tiled=True)
    key_docs = lax.all_gather(doc_ids, "seq", axis=0, tiled=True)
    key_pos = jnp.arange(keys.shape[0], dtype=jnp.int32)
    key_heads = to_heads(keys)
    value_heads = to_heads(values)
    updated = []
    for member, state in zip(prepared, initial):
        queries, query_pos, query_docs = member

        def advance(inner, queries=queries, query_pos=query_pos, query_docs=query_docs):
            return attend_block(
                inner, queries, query_pos, query_docs, key_heads, value_heads, key_pos, key_docs
            )

        def unchanged(inner):
            return inner

        updated.append(lax.cond(first_row <= jnp.max(query_pos), advance, unchanged, state))
    finals = tuple(updated)
    outputs = []
    for run_max, run_sum, run_acc in finals:
        normed = run_acc / run_sum[..., None]
        outputs.append(
            jnp.transpose(normed, (1, 0, 2))
            .reshape(normed.shape[1], heads * HEAD_DIM)
            .astype(jnp.bfloat16)
        )
    attended = outputs[0]
    mapped = jnp.dot(
        attended,
        lax.all_gather(out_weight, "seq", axis=1, tiled=True),
        preferred_element_type=jnp.float32,
    )
    summed = lax.psum_scatter(mapped, "head", scatter_dimension=1, tiled=True)
    return (residual.astype(jnp.float32) + summed).astype(jnp.bfloat16)


MESH = pl.DeviceIdType.MESH


STEPS = 2
PIECES = 4


def attention(queries, keys, values, doc_row, row_pos):
    rows, keep = queries.shape[0], keys.shape[0]
    scores = lax.dot_general(
        queries, keys, (((1,), (1,)), ((), ())), preferred_element_type=jnp.float32
    ) * HEAD_DIM ** (-0.5)
    col_pos = lax.broadcasted_iota(jnp.int32, (rows, keep), 1)
    docs = jnp.broadcast_to(doc_row, (rows, keep))
    query_docs = jnp.sum(jnp.where(row_pos == col_pos, docs, 0.0), axis=1, keepdims=True)
    allowed = (col_pos <= row_pos) & (docs == query_docs)
    scores = jnp.where(allowed, scores, masked_score)
    row_max = jnp.max(scores, axis=1, keepdims=True)
    weights = jnp.where(allowed, jnp.exp(scores - row_max), 0.0)
    row_sum = jnp.sum(weights, axis=1, keepdims=True)
    product = jnp.dot(weights.astype(jnp.bfloat16), values, preferred_element_type=jnp.float32)
    return (product / row_sum).astype(jnp.bfloat16)


def fused_kernel(
    nz, q_ref, k_ref, v_ref, doc_ref, w_ref, res_ref, out_ref,
    stage, docin, inbox, mine, att, wbuf, sendbuf, parts, resbuf,
    in_sem, i_send, i_recv, b_send, b_recv, z_send, z_recv, f_send, f_recv,
    p_send, p_recv, w_send, w_recv, res_sem,
):
    me = lax.axis_index("seq")
    head = lax.axis_index("head")
    rows = k_ref.shape[0]
    z, y = me // 2, me % 2
    x, core = head // 2, head % 2
    wrows = w_ref.shape[0]
    wcols = w_ref.shape[1]

    tall = stage.shape[0]
    chunk = wrows // PIECES

    def peer(to):
        return 2 * to + y, head

    def greet(to):
        pl.semaphore_signal(barrier, inc=1, device_id=to, device_id_type=MESH)

    barrier = pltpu.get_barrier_semaphore()
    for dz in range(1, nz):
        greet(peer(lax.rem(z + dz, nz)))
    for dy in range(2):
        for dh in range(4):
            if dy or dh:
                greet((2 * z + lax.rem(y + dy, 2), lax.rem(head + dh, 4)))

    def arrived(ref, sem):
        pltpu.make_async_copy(ref, ref, sem).wait()

    staged = [
        pltpu.make_async_copy(src, dst, in_sem.at[index])
        for index, (src, dst) in enumerate((
            (doc_ref, docin),
            (q_ref, stage.at[pl.ds(0, rows), :]),
            (k_ref, stage.at[pl.ds(rows, rows), :]),
            (v_ref, stage.at[pl.ds(2 * rows, rows), :]),
        ))
    ]
    for copy in staged:
        copy.start()
    res_copy = pltpu.make_async_copy(res_ref, resbuf, res_sem)
    res_copy.start()

    def remote(src, dst, send, recv, to):
        return pltpu.make_async_remote_copy(
            src_ref=src, dst_ref=dst, send_sem=send, recv_sem=recv,
            device_id=to, device_id_type=MESH,
        )

    def start(copy):
        copy.start()

    def sent(copy):
        copy.wait_send()

    def by_distance(act, far_first=False):
        order = [(0, 0)] + [(far, step) for far in range(1, nz) for step in (far, -far)]
        for far, step in reversed(order) if far_first else order:
            @pl.when((z + step >= 0) & (z + step < nz))
            def _(step=step):
                act(z + step)

    def to_peer(to, src, dst, send, recv, act, act_own):
        own = to == z

        @pl.when(jnp.logical_not(own))
        def _():
            act(remote(src, dst, send, recv, peer(to)))

        if act_own:
            @pl.when(own)
            def _():
                act_own(pltpu.make_async_copy(src, dst, recv))

    partner = (me, 2 * x + 1 - core)

    def hand_out(to, act, act_own=None):
        lanes = pl.ds(pl.multiple_of(to * HEAD_DIM, HEAD_DIM), HEAD_DIM)
        to_peer(
            to, stage.at[:, lanes], inbox.at[me], i_send.at[to], i_recv.at[z], act, act_own
        )

    def share(source):
        ref = inbox.at[2 * source + y, pl.ds(rows, tall - rows), :]
        return remote(
            ref, ref, b_send.at[source], b_recv.at[source], (2 * z + 1 - y, head)
        )

    staged[0].wait()
    numbers = jnp.broadcast_to(docin[...].astype(jnp.float32), (tall - 3 * rows, rows))
    if rows < HEAD_DIM:
        blank = jnp.zeros((tall - 3 * rows, HEAD_DIM - rows), jnp.float32)
        numbers = jnp.concatenate([numbers, blank], axis=1)
    for index in range(nz):
        stage[3 * rows:, index * HEAD_DIM:(index + 1) * HEAD_DIM] = numbers.astype(jnp.bfloat16)
    for copy in staged[1:]:
        copy.wait()

    def w_part(piece):
        src = w_ref.at[pl.ds(piece * chunk, chunk), :]
        dst = wbuf.at[pl.ds(pl.multiple_of(core * wrows + piece * chunk, chunk), chunk), :]
        recv = w_recv.at[core, piece]
        return (
            pltpu.make_async_copy(src, dst, recv),
            remote(src, dst, w_send.at[0, piece], recv, (2 * z + 1 - y, 2 * x + y)),
            remote(src, dst, w_send.at[1, piece], recv, (me, 2 * x + y)),
        )

    def w_start(piece):
        kept, across, beside = w_part(piece)
        across.start()

        @pl.when(core == y)
        def _():
            kept.start()

        @pl.when(core != y)
        def _():
            beside.start()

    pl.semaphore_wait(barrier, nz + 6)

    by_distance(lambda to: hand_out(to, start, start))
    w_start(0)

    deep = nz // STEPS
    part = deep * rows
    row_id = lax.broadcasted_iota(jnp.int32, (part, 1), 0)
    row_pos = row_id + y * rows
    for index in range(1, deep):
        row_pos = row_pos + jnp.where(row_id >= index * rows, rows, 0)

    def att_part(c, source, step):
        return att.at[c * nz + source, pl.ds(step * part, part), :]

    def along(to, step, act, act_own=None):
        to_peer(
            to, mine.at[pl.ds(step * part, part), :], att_part(core, z, step),
            z_send.at[to, step], z_recv.at[z, step], act, act_own,
        )

    def forward(source, step):
        ref = att_part(core, source, step)
        return remote(ref, ref, f_send.at[source, step], f_recv.at[source, step], partner)

    def receive(source):
        arrived(inbox.at[2 * source + y], i_recv.at[source])
        share(source).start()

    by_distance(receive)
    for piece in range(1, 2):
        w_start(piece)

    for step in range(STEPS):
        for source in range(deep * step, deep * (step + 1)):
            arrived(
                inbox.at[2 * source + 1 - y, pl.ds(rows, tall - rows), :], b_recv.at[source]
            )
        seen = range(2 * deep * (step + 1))
        mine[step * part:(step + 1) * part, :] = attention(
            jnp.concatenate(
                [inbox[2 * k + y, :rows, :] for k in range(deep * step, deep * (step + 1))],
                axis=0,
            ),
            jnp.concatenate([inbox[source, rows:2 * rows, :] for source in seen], axis=0),
            jnp.concatenate([inbox[source, 2 * rows:3 * rows, :] for source in seen], axis=0),
            jnp.concatenate(
                [inbox[source, 3 * rows:, :].astype(jnp.float32)[:1, :rows] for source in seen],
                axis=1,
            ),
            row_pos + 2 * part * step,
        )
        by_distance(lambda to, step=step: along(to, step, start, start), far_first=True)
        if step == 0:
            for piece in range(2, 4):
                w_start(piece)

    slot = 2 * x + core

    def deliver(block, act, act_own=None):
        own = (me == 2 * block + y) & (head == z)
        src = sendbuf.at[pl.ds(block * rows, rows), :]

        if act_own:
            @pl.when(own)
            def _():
                act_own(pltpu.make_async_copy(src, parts.at[slot], p_recv.at[slot]))

        @pl.when(jnp.logical_not(own))
        def _():
            act(remote(
                src, parts.at[slot], p_send.at[block], p_recv.at[slot], (2 * block + y, z)
            ))

    def pass_on(step):
        def one(source):
            arrived(att_part(core, source, step), z_recv.at[source, step])
            forward(source, step).start()

        by_distance(one)

    pass_on(0)

    @pl.when(core != y)
    def _():
        for step in range(1, STEPS):
            pass_on(step)

    for step in range(STEPS):
        if step:
            @pl.when(core == y)
            def _(step=step):
                pass_on(step)

        for source in range(nz):
            arrived(att_part(1 - core, source, step), f_recv.at[source, step])
        if step == 0:
            for index in range(2):
                for piece in range(PIECES):
                    arrived(
                        wbuf.at[pl.ds(index * wrows + piece * chunk, chunk), :],
                        w_recv.at[index, piece],
                    )
        attended = jnp.concatenate(
            [att[index, step * part:(step + 1) * part, :] for index in range(2 * nz)], axis=1
        )
        sendbuf[step * part:(step + 1) * part, :] = jnp.dot(
            attended, wbuf[...], preferred_element_type=jnp.float32
        ).astype(jnp.bfloat16)
        for block in range(deep * step, deep * (step + 1)):
            deliver(block if step == 0 else deep * (2 * step + 1) - 1 - block, start, start)

    res_copy.wait()
    for c in range(2):
        for p in range(2):
            arrived(parts.at[2 * p + c], p_recv.at[2 * p + c])
        cols = slice(c * wcols, (c + 1) * wcols)
        total = parts[c].astype(jnp.float32) + parts[2 + c].astype(jnp.float32)
        out_ref[:, cols] = (resbuf[:, cols].astype(jnp.float32) + total).astype(jnp.bfloat16)

    by_distance(lambda to: hand_out(to, sent))
    for source in range(nz):
        share(source).wait_send()
    for piece in range(PIECES):
        _, across, beside = w_part(piece)
        across.wait_send()

        @pl.when(core != y)
        def _(beside=beside):
            beside.wait_send()

    for step in range(STEPS):
        by_distance(lambda to, step=step: along(to, step, sent))
        for source in range(nz):
            forward(source, step).wait_send()
    for block in range(nz):
        deliver(block, sent)


def fused(n, query, key_states, value_states, doc_ids, out_weight, residual):
    rows, width = key_states.shape
    wrows, wcols = out_weight.shape
    seq, nz = n * rows, n // 2
    dma = pltpu.SemaphoreType.DMA
    any_ = pl.BlockSpec(memory_space=pl.ANY)
    bf16 = jnp.bfloat16
    return pl.pallas_call(
        functools.partial(fused_kernel, nz),
        out_shape=jax.ShapeDtypeStruct(residual.shape, residual.dtype),
        in_specs=[any_] * 6,
        out_specs=pl.BlockSpec(memory_space=pltpu.VMEM),
        scratch_shapes=[
            pltpu.VMEM((3 * rows + 16, width), bf16),
            pltpu.VMEM((1, rows), jnp.int32),
            pltpu.VMEM((n, 3 * rows + 16, HEAD_DIM), bf16),
            pltpu.VMEM((seq // 2, HEAD_DIM), bf16),
            pltpu.VMEM((n, seq // 2, HEAD_DIM), bf16),
            pltpu.VMEM((2 * wrows, wcols), bf16),
            pltpu.VMEM((seq // 2, wcols), bf16),
            pltpu.VMEM((4, rows, wcols), bf16),
            pltpu.VMEM(residual.shape, bf16),
            dma((4,)),
            dma((nz,)), dma((nz,)),
            dma((nz,)), dma((nz,)),
            dma((nz, STEPS)), dma((nz, STEPS)),
            dma((nz, STEPS)), dma((nz, STEPS)),
            dma((nz,)), dma((4,)),
            dma((2, PIECES)), dma((2, PIECES)), dma,
        ],
        compiler_params=pltpu.CompilerParams(collective_id=0, has_side_effects=True),
    )(query, key_states, value_states, doc_ids.reshape(1, rows), out_weight, residual)


def solution(mesh):
    placed = (
        P("seq", "head"),
        P("seq", "head"),
        P("seq", "head"),
        P("seq"),
        P("head", "seq"),
        P("seq", "head"),
    )
    n, nh = mesh.shape["seq"], mesh.shape["head"]

    def body(query, key_states, value_states, doc_ids, out_weight, residual):
        heads = query.shape[1] // HEAD_DIM
        fits = (
            n == 2 * heads
            and n == 2 * nh
            and nh == 4
            and out_weight.shape[0] % (16 * PIECES) == 0
            and out_weight.shape[1] % 256 == 0
            and query.shape[0] % 16 == 0
            and query.shape[0] <= HEAD_DIM
        )
        run = functools.partial(fused, n) if fits else shards
        return run(query, key_states, value_states, doc_ids, out_weight, residual)

    return jax.shard_map(
        body, mesh=mesh, in_specs=placed, out_specs=P("seq", "head"), check_vma=False
    )
```

```python
import functools

import jax
import jax.numpy as jnp
from jax import lax
from jax.experimental import pallas as pl
from jax.experimental.pallas import tpu as pltpu
from jax.sharding import PartitionSpec as P

HEAD_DIM = 128


masked_score = -1e30


def to_heads(block):
    return block.reshape(block.shape[0], block.shape[1] // HEAD_DIM, HEAD_DIM)


def attend_block(state, queries, query_pos, query_docs, keys, values, key_pos, key_docs):
    run_max, run_sum, run_acc = state
    scores = jnp.einsum(
        "qhd,khd->hqk", queries, keys, preferred_element_type=jnp.float32
    ) * HEAD_DIM ** (-0.5)
    allowed = (key_pos[None, :] <= query_pos[:, None]) & (key_docs[None, :] == query_docs[:, None])
    scores = jnp.where(allowed[None], scores, masked_score)
    new_max = jnp.maximum(run_max, jnp.max(scores, axis=-1))
    weights = jnp.where(allowed[None], jnp.exp(scores - new_max[..., None]), 0.0)
    run_sum = jnp.sum(weights, axis=-1)
    run_acc = jnp.einsum(
        "hqk,khd->hqd", weights.astype(jnp.bfloat16), values, preferred_element_type=jnp.float32
    )
    return (new_max, run_sum, run_acc)


def shards(query, key_states, value_states, doc_ids, out_weight, residual):
    tok_rows = query.shape[0]
    heads = query.shape[1] // HEAD_DIM
    shard_index = lax.axis_index("seq")
    first_pos = shard_index * tok_rows
    groups = [(query, first_pos + jnp.arange(tok_rows, dtype=jnp.int32), doc_ids)]
    prepared = [(to_heads(block), block_pos, block_docs) for block, block_pos, block_docs in groups]
    initial = tuple(
        (
            (
                jnp.full((heads, block_pos.shape[0]), masked_score, jnp.float32),
                jnp.zeros((heads, block_pos.shape[0]), jnp.float32),
                jnp.zeros((heads, block_pos.shape[0], HEAD_DIM), jnp.float32),
            )
            for block, block_pos, block_docs in groups
        )
    )
    first_row = jnp.int32(0)
    keys = lax.all_gather(key_states, "seq", axis=0, tiled=True)
    values = lax.all_gather(value_states, "seq", axis=0, tiled=True)
    key_docs = lax.all_gather(doc_ids, "seq", axis=0, tiled=True)
    key_pos = jnp.arange(keys.shape[0], dtype=jnp.int32)
    key_heads = to_heads(keys)
    value_heads = to_heads(values)
    updated = []
    for member, state in zip(prepared, initial):
        queries, query_pos, query_docs = member

        def advance(inner, queries=queries, query_pos=query_pos, query_docs=query_docs):
            return attend_block(
                inner, queries, query_pos, query_docs, key_heads, value_heads, key_pos, key_docs
            )

        def unchanged(inner):
            return inner

        updated.append(lax.cond(first_row <= jnp.max(query_pos), advance, unchanged, state))
    finals = tuple(updated)
    outputs = []
    for run_max, run_sum, run_acc in finals:
        normed = run_acc / run_sum[..., None]
        outputs.append(
            jnp.transpose(normed, (1, 0, 2))
            .reshape(normed.shape[1], heads * HEAD_DIM)
            .astype(jnp.bfloat16)
        )
    attended = outputs[0]
    mapped = jnp.dot(
        attended,
        lax.all_gather(out_weight, "seq", axis=1, tiled=True),
        preferred_element_type=jnp.float32,
    )
    summed = lax.psum_scatter(mapped, "head", scatter_dimension=1, tiled=True)
    return (residual.astype(jnp.float32) + summed).astype(jnp.bfloat16)


MESH = pl.DeviceIdType.MESH


STEPS = 2
PIECES = 4


def attention(queries, keys, values, doc_row, row_pos):
    rows, keep = queries.shape[0], keys.shape[0]
    scores = lax.dot_general(
        queries, keys, (((1,), (1,)), ((), ())), preferred_element_type=jnp.float32
    ) * HEAD_DIM ** (-0.5)
    col_pos = lax.broadcasted_iota(jnp.int32, (rows, keep), 1)
    docs = jnp.broadcast_to(doc_row, (rows, keep))
    query_docs = jnp.sum(jnp.where(row_pos == col_pos, docs, 0.0), axis=1, keepdims=True)
    allowed = (col_pos <= row_pos) & (docs == query_docs)
    scores = jnp.where(allowed, scores, masked_score)
    row_max = jnp.max(scores, axis=1, keepdims=True)
    weights = jnp.where(allowed, jnp.exp(scores - row_max), 0.0)
    row_sum = jnp.sum(weights, axis=1, keepdims=True)
    product = jnp.dot(weights.astype(jnp.bfloat16), values, preferred_element_type=jnp.float32)
    return (product / row_sum).astype(jnp.bfloat16)


def fused_kernel(
    nz, q_ref, k_ref, v_ref, doc_ref, w_ref, res_ref, out_ref,
    stage, docin, inbox, mine, att, wbuf, sendbuf, parts, resbuf,
    in_sem, i_send, i_recv, b_send, b_recv, z_send, z_recv, f_send, f_recv,
    p_send, p_recv, w_send, w_recv, res_sem,
):
    me = lax.axis_index("seq")
    head = lax.axis_index("head")
    rows = k_ref.shape[0]
    z, y = me // 2, me % 2
    x, core = head // 2, head % 2
    wrows = w_ref.shape[0]
    wcols = w_ref.shape[1]

    tall = stage.shape[0]
    chunk = wrows // PIECES

    def peer(to):
        return 2 * to + y, head

    def greet(to):
        pl.semaphore_signal(barrier, inc=1, device_id=to, device_id_type=MESH)

    barrier = pltpu.get_barrier_semaphore()
    for dz in range(1, nz):
        greet(peer(lax.rem(z + dz, nz)))
    for dy in range(2):
        for dh in range(4):
            if dy or dh:
                greet((2 * z + lax.rem(y + dy, 2), lax.rem(head + dh, 4)))

    def arrived(ref, sem):
        pltpu.make_async_copy(ref, ref, sem).wait()

    staged = [
        pltpu.make_async_copy(src, dst, in_sem.at[index])
        for index, (src, dst) in enumerate((
            (doc_ref, docin),
            (q_ref, stage.at[pl.ds(0, rows), :]),
            (k_ref, stage.at[pl.ds(rows, rows), :]),
            (v_ref, stage.at[pl.ds(2 * rows, rows), :]),
        ))
    ]
    for copy in staged:
        copy.start()
    res_copy = pltpu.make_async_copy(res_ref, resbuf, res_sem)
    res_copy.start()

    def remote(src, dst, send, recv, to):
        return pltpu.make_async_remote_copy(
            src_ref=src, dst_ref=dst, send_sem=send, recv_sem=recv,
            device_id=to, device_id_type=MESH,
        )

    def start(copy):
        copy.start()

    def sent(copy):
        copy.wait_send()

    def by_distance(act, far_first=False):
        order = [(0, 0)] + [(far, step) for far in range(1, nz) for step in (far, -far)]
        for far, step in reversed(order) if far_first else order:
            @pl.when((z + step >= 0) & (z + step < nz))
            def _(step=step):
                act(z + step)

    def to_peer(to, src, dst, send, recv, act, act_own):
        own = to == z

        @pl.when(jnp.logical_not(own))
        def _():
            act(remote(src, dst, send, recv, peer(to)))

        if act_own:
            @pl.when(own)
            def _():
                act_own(pltpu.make_async_copy(src, dst, recv))

    partner = (me, 2 * x + 1 - core)

    def hand_out(to, act, act_own=None):
        lanes = pl.ds(pl.multiple_of(to * HEAD_DIM, HEAD_DIM), HEAD_DIM)
        to_peer(
            to, stage.at[:, lanes], inbox.at[me], i_send.at[to], i_recv.at[z], act, act_own
        )

    def share(source):
        ref = inbox.at[2 * source + y, pl.ds(rows, tall - rows), :]
        return remote(
            ref, ref, b_send.at[source], b_recv.at[source], (2 * z + 1 - y, head)
        )

    staged[0].wait()
    numbers = jnp.broadcast_to(docin[...].astype(jnp.float32), (tall - 3 * rows, rows))
    if rows < HEAD_DIM:
        blank = jnp.zeros((tall - 3 * rows, HEAD_DIM - rows), jnp.float32)
        numbers = jnp.concatenate([numbers, blank], axis=1)
    for index in range(nz):
        stage[3 * rows:, index * HEAD_DIM:(index + 1) * HEAD_DIM] = numbers.astype(jnp.bfloat16)
    for copy in staged[1:]:
        copy.wait()

    def w_part(piece):
        src = w_ref.at[pl.ds(piece * chunk, chunk), :]
        dst = wbuf.at[pl.ds(pl.multiple_of(core * wrows + piece * chunk, chunk), chunk), :]
        recv = w_recv.at[core, piece]
        return (
            pltpu.make_async_copy(src, dst, recv),
            remote(src, dst, w_send.at[0, piece], recv, (2 * z + 1 - y, 2 * x + y)),
            remote(src, dst, w_send.at[1, piece], recv, (me, 2 * x + y)),
        )

    def w_start(piece):
        kept, across, beside = w_part(piece)
        across.start()

        @pl.when(core == y)
        def _():
            kept.start()

        @pl.when(core != y)
        def _():
            beside.start()

    pl.semaphore_wait(barrier, nz + 6)

    by_distance(lambda to: hand_out(to, start, start))
    w_start(0)

    deep = nz // STEPS
    part = deep * rows
    row_id = lax.broadcasted_iota(jnp.int32, (part, 1), 0)
    row_pos = row_id + y * rows
    for index in range(1, deep):
        row_pos = row_pos + jnp.where(row_id >= index * rows, rows, 0)

    def att_part(c, source, step):
        return att.at[c * nz + source, pl.ds(step * part, part), :]

    def along(to, step, act, act_own=None):
        to_peer(
            to, mine.at[pl.ds(step * part, part), :], att_part(core, z, step),
            z_send.at[to, step], z_recv.at[z, step], act, act_own,
        )

    def forward(source, step):
        ref = att_part(core, source, step)
        return remote(ref, ref, f_send.at[source, step], f_recv.at[source, step], partner)

    def receive(source):
        arrived(inbox.at[2 * source + y], i_recv.at[source])
        share(source).start()

    by_distance(receive)
    for piece in range(1, 2):
        w_start(piece)

    for step in range(STEPS):
        for source in range(deep * step, deep * (step + 1)):
            arrived(
                inbox.at[2 * source + 1 - y, pl.ds(rows, tall - rows), :], b_recv.at[source]
            )
        seen = range(2 * deep * (step + 1))
        mine[step * part:(step + 1) * part, :] = attention(
            jnp.concatenate(
                [inbox[2 * k + y, :rows, :] for k in range(deep * step, deep * (step + 1))],
                axis=0,
            ),
            jnp.concatenate([inbox[source, rows:2 * rows, :] for source in seen], axis=0),
            jnp.concatenate([inbox[source, 2 * rows:3 * rows, :] for source in seen], axis=0),
            jnp.concatenate(
                [inbox[source, 3 * rows:, :].astype(jnp.float32)[:1, :rows] for source in seen],
                axis=1,
            ),
            row_pos + 2 * part * step,
        )
        by_distance(lambda to, step=step: along(to, step, start, start), far_first=True)
        if step == 0:
            for piece in range(2, 4):
                w_start(piece)

    slot = 2 * x + core

    def deliver(block, act, act_own=None):
        own = (me == 2 * block + y) & (head == z)
        src = sendbuf.at[pl.ds(block * rows, rows), :]

        if act_own:
            @pl.when(own)
            def _():
                act_own(pltpu.make_async_copy(src, parts.at[slot], p_recv.at[slot]))

        @pl.when(jnp.logical_not(own))
        def _():
            act(remote(
                src, parts.at[slot], p_send.at[block], p_recv.at[slot], (2 * block + y, z)
            ))

    def pass_on(step):
        def one(source):
            arrived(att_part(core, source, step), z_recv.at[source, step])
            forward(source, step).start()

        by_distance(one)

    pass_on(0)

    @pl.when(core != y)
    def _():
        for step in range(1, STEPS):
            pass_on(step)

    for step in range(STEPS):
        if step:
            @pl.when(core == y)
            def _(step=step):
                pass_on(step)

        for source in range(nz):
            arrived(att_part(1 - core, source, step), f_recv.at[source, step])
        if step == 0:
            for index in range(2):
                for piece in range(PIECES):
                    arrived(
                        wbuf.at[pl.ds(index * wrows + piece * chunk, chunk), :],
                        w_recv.at[index, piece],
                    )
        attended = jnp.concatenate(
            [att[index, step * part:(step + 1) * part, :] for index in range(2 * nz)], axis=1
        )
        sendbuf[step * part:(step + 1) * part, :] = jnp.dot(
            attended, wbuf[...], preferred_element_type=jnp.float32
        ).astype(jnp.bfloat16)
        for block in range(deep * step, deep * (step + 1)):
            deliver(block if step == 0 else deep * (2 * step + 1) - 1 - block, start, start)

    res_copy.wait()
    for c in range(2):
        for p in range(2):
            arrived(parts.at[2 * p + c], p_recv.at[2 * p + c])
        cols = slice(c * wcols, (c + 1) * wcols)
        total = parts[c].astype(jnp.float32) + parts[2 + c].astype(jnp.float32)
        out_ref[:, cols] = (resbuf[:, cols].astype(jnp.float32) + total).astype(jnp.bfloat16)

    by_distance(lambda to: hand_out(to, sent))
    for source in range(nz):
        share(source).wait_send()
    for piece in range(PIECES):
        _, across, beside = w_part(piece)
        across.wait_send()

        @pl.when(core != y)
        def _(beside=beside):
            beside.wait_send()

    for step in range(STEPS):
        by_distance(lambda to, step=step: along(to, step, sent))
        for source in range(nz):
            forward(source, step).wait_send()
    for block in range(nz):
        deliver(block, sent)


def fused(n, query, key_states, value_states, doc_ids, out_weight, residual):
    rows, width = key_states.shape
    wrows, wcols = out_weight.shape
    seq, nz = n * rows, n // 2
    dma = pltpu.SemaphoreType.DMA
    any_ = pl.BlockSpec(memory_space=pl.ANY)
    bf16 = jnp.bfloat16
    return pl.pallas_call(
        functools.partial(fused_kernel, nz),
        out_shape=jax.ShapeDtypeStruct(residual.shape, residual.dtype),
        in_specs=[any_] * 6,
        out_specs=pl.BlockSpec(memory_space=pltpu.VMEM),
        scratch_shapes=[
            pltpu.VMEM((3 * rows + 16, width), bf16),
            pltpu.VMEM((1, rows), jnp.int32),
            pltpu.VMEM((n, 3 * rows + 16, HEAD_DIM), bf16),
            pltpu.VMEM((seq // 2, HEAD_DIM), bf16),
            pltpu.VMEM((n, seq // 2, HEAD_DIM), bf16),
            pltpu.VMEM((2 * wrows, wcols), bf16),
            pltpu.VMEM((seq // 2, wcols), bf16),
            pltpu.VMEM((4, rows, wcols), bf16),
            pltpu.VMEM(residual.shape, bf16),
            dma((4,)),
            dma((nz,)), dma((nz,)),
            dma((nz,)), dma((nz,)),
            dma((nz, STEPS)), dma((nz, STEPS)),
            dma((nz, STEPS)), dma((nz, STEPS)),
            dma((nz,)), dma((4,)),
            dma((2, PIECES)), dma((2, PIECES)), dma,
        ],
        compiler_params=pltpu.CompilerParams(collective_id=0, has_side_effects=True, vmem_limit_bytes=16 << 20),
    )(*[pltpu.with_memory_space_constraint(a, pltpu.HBM) for a in (query, key_states, value_states, doc_ids.reshape(1, rows), out_weight, residual)])


def solution(mesh):
    placed = (
        P("seq", "head"),
        P("seq", "head"),
        P("seq", "head"),
        P("seq"),
        P("head", "seq"),
        P("seq", "head"),
    )
    n, nh = mesh.shape["seq"], mesh.shape["head"]

    def body(query, key_states, value_states, doc_ids, out_weight, residual):
        heads = query.shape[1] // HEAD_DIM
        fits = (
            n == 2 * heads
            and n == 2 * nh
            and nh == 4
            and out_weight.shape[0] % (16 * PIECES) == 0
            and out_weight.shape[1] % 256 == 0
            and query.shape[0] % 16 == 0
            and query.shape[0] <= HEAD_DIM
        )
        run = functools.partial(fused, n) if fits else shards
        return run(query, key_states, value_states, doc_ids, out_weight, residual)

    return jax.shard_map(
        body, mesh=mesh, in_specs=placed, out_specs=P("seq", "head"), check_vma=False
    )
```

```python
import functools

import jax
import jax.numpy as jnp
from jax import lax
from jax.experimental import pallas as pl
from jax.experimental.pallas import tpu as pltpu
from jax.sharding import PartitionSpec as P

HEAD_DIM = 128


masked_score = -1e30


def to_heads(block):
    return block.reshape(block.shape[0], block.shape[1] // HEAD_DIM, HEAD_DIM)


def attend_block(state, queries, query_pos, query_docs, keys, values, key_pos, key_docs):
    run_max, run_sum, run_acc = state
    scores = jnp.einsum(
        "qhd,khd->hqk", queries, keys, preferred_element_type=jnp.float32
    ) * HEAD_DIM ** (-0.5)
    allowed = (key_pos[None, :] <= query_pos[:, None]) & (key_docs[None, :] == query_docs[:, None])
    scores = jnp.where(allowed[None], scores, masked_score)
    new_max = jnp.maximum(run_max, jnp.max(scores, axis=-1))
    weights = jnp.where(allowed[None], jnp.exp(scores - new_max[..., None]), 0.0)
    run_sum = jnp.sum(weights, axis=-1)
    run_acc = jnp.einsum(
        "hqk,khd->hqd", weights.astype(jnp.bfloat16), values, preferred_element_type=jnp.float32
    )
    return (new_max, run_sum, run_acc)


def shards(query, key_states, value_states, doc_ids, out_weight, residual):
    tok_rows = query.shape[0]
    heads = query.shape[1] // HEAD_DIM
    shard_index = lax.axis_index("seq")
    first_pos = shard_index * tok_rows
    groups = [(query, first_pos + jnp.arange(tok_rows, dtype=jnp.int32), doc_ids)]
    prepared = [(to_heads(block), block_pos, block_docs) for block, block_pos, block_docs in groups]
    initial = tuple(
        (
            (
                jnp.full((heads, block_pos.shape[0]), masked_score, jnp.float32),
                jnp.zeros((heads, block_pos.shape[0]), jnp.float32),
                jnp.zeros((heads, block_pos.shape[0], HEAD_DIM), jnp.float32),
            )
            for block, block_pos, block_docs in groups
        )
    )
    first_row = jnp.int32(0)
    keys = lax.all_gather(key_states, "seq", axis=0, tiled=True)
    values = lax.all_gather(value_states, "seq", axis=0, tiled=True)
    key_docs = lax.all_gather(doc_ids, "seq", axis=0, tiled=True)
    key_pos = jnp.arange(keys.shape[0], dtype=jnp.int32)
    key_heads = to_heads(keys)
    value_heads = to_heads(values)
    updated = []
    for member, state in zip(prepared, initial):
        queries, query_pos, query_docs = member

        def advance(inner, queries=queries, query_pos=query_pos, query_docs=query_docs):
            return attend_block(
                inner, queries, query_pos, query_docs, key_heads, value_heads, key_pos, key_docs
            )

        def unchanged(inner):
            return inner

        updated.append(lax.cond(first_row <= jnp.max(query_pos), advance, unchanged, state))
    finals = tuple(updated)
    outputs = []
    for run_max, run_sum, run_acc in finals:
        normed = run_acc / run_sum[..., None]
        outputs.append(
            jnp.transpose(normed, (1, 0, 2))
            .reshape(normed.shape[1], heads * HEAD_DIM)
            .astype(jnp.bfloat16)
        )
    attended = outputs[0]
    mapped = jnp.dot(
        attended,
        lax.all_gather(out_weight, "seq", axis=1, tiled=True),
        preferred_element_type=jnp.float32,
    )
    summed = lax.psum_scatter(mapped, "head", scatter_dimension=1, tiled=True)
    return (residual.astype(jnp.float32) + summed).astype(jnp.bfloat16)


MESH = pl.DeviceIdType.MESH


STEPS = 2
PIECES = 8
W_PLAN = ((3, 2, 3, 0), (2, 0, 2, 4))


def attention(queries, keys, values, doc_row, row_pos):
    rows, keep = queries.shape[0], keys.shape[0]
    scores = lax.dot_general(
        queries, keys, (((1,), (1,)), ((), ())), preferred_element_type=jnp.float32
    ) * HEAD_DIM ** (-0.5)
    col_pos = lax.broadcasted_iota(jnp.int32, (rows, keep), 1)
    docs = jnp.broadcast_to(doc_row, (rows, keep))
    query_docs = jnp.sum(jnp.where(row_pos == col_pos, docs, 0.0), axis=1, keepdims=True)
    allowed = (col_pos <= row_pos) & (docs == query_docs)
    scores = jnp.where(allowed, scores, masked_score)
    row_max = jnp.max(scores, axis=1, keepdims=True)
    weights = jnp.where(allowed, jnp.exp(scores - row_max), 0.0)
    row_sum = jnp.sum(weights, axis=1, keepdims=True)
    product = jnp.dot(weights.astype(jnp.bfloat16), values, preferred_element_type=jnp.float32)
    return (product / row_sum).astype(jnp.bfloat16)


def fused_kernel(
    nz, q_ref, k_ref, v_ref, doc_ref, w_ref, res_ref, out_ref,
    stage, docin, inbox, docbuf, mine, att, wbuf, sendbuf, parts, resbuf,
    in_sem, i_send, i_recv, b_send, b_recv, d_send, d_recv, e_send, e_recv, z_send, z_recv, f_send, f_recv,
    p_send, p_recv, w_send, w_recv, res_sem,
):
    me = lax.axis_index("seq")
    head = lax.axis_index("head")
    rows = k_ref.shape[0]
    z, y = me // 2, me % 2
    x, core = head // 2, head % 2
    wrows = w_ref.shape[0]
    wcols = w_ref.shape[1]

    tall = stage.shape[0]
    chunk = wrows // PIECES

    def peer(to):
        return 2 * to + y, head

    def greet(to):
        pl.semaphore_signal(barrier, inc=1, device_id=to, device_id_type=MESH)

    barrier = pltpu.get_barrier_semaphore()
    for dz in range(1, nz):
        greet(peer(lax.rem(z + dz, nz)))
    for dy in range(2):
        for dh in range(4):
            if dy or dh:
                greet((2 * z + lax.rem(y + dy, 2), lax.rem(head + dh, 4)))

    def arrived(ref, sem):
        pltpu.make_async_copy(ref, ref, sem).wait()

    staged = [
        pltpu.make_async_copy(src, dst, in_sem.at[index])
        for index, (src, dst) in enumerate((
            (doc_ref, docin),
            (q_ref, stage.at[pl.ds(0, rows), :]),
            (k_ref, stage.at[pl.ds(rows, rows), :]),
            (v_ref, stage.at[pl.ds(2 * rows, rows), :]),
        ))
    ]
    for copy in staged:
        copy.start()
    res_copy = pltpu.make_async_copy(res_ref, resbuf, res_sem)
    res_copy.start()

    def remote(src, dst, send, recv, to):
        return pltpu.make_async_remote_copy(
            src_ref=src, dst_ref=dst, send_sem=send, recv_sem=recv,
            device_id=to, device_id_type=MESH,
        )

    def start(copy):
        copy.start()

    def sent(copy):
        copy.wait_send()

    def by_distance(act, far_first=False):
        order = [(0, 0)] + [(far, step) for far in range(1, nz) for step in (far, -far)]
        for far, step in reversed(order) if far_first else order:
            @pl.when((z + step >= 0) & (z + step < nz))
            def _(step=step):
                act(z + step)

    def to_peer(to, src, dst, send, recv, act, act_own):
        own = to == z

        @pl.when(jnp.logical_not(own))
        def _():
            act(remote(src, dst, send, recv, peer(to)))

        if act_own:
            @pl.when(own)
            def _():
                act_own(pltpu.make_async_copy(src, dst, recv))

    partner = (me, 2 * x + 1 - core)

    def hand_out(to, act, act_own=None):
        lanes = pl.ds(pl.multiple_of(to * HEAD_DIM, HEAD_DIM), HEAD_DIM)
        to_peer(to, docin, docbuf.at[me], d_send.at[to], d_recv.at[z], act, act_own)
        to_peer(
            to, stage.at[:, lanes], inbox.at[me], i_send.at[to], i_recv.at[z], act, act_own
        )

    def share(source, act):
        ref = inbox.at[2 * source + y, pl.ds(rows, tall - rows), :]
        numbers = docbuf.at[2 * source + y]
        to = (2 * z + 1 - y, head)
        act(remote(numbers, numbers, e_send.at[source], e_recv.at[source], to))
        act(remote(ref, ref, b_send.at[source], b_recv.at[source], to))

    for copy in staged:
        copy.wait()

    def w_part(piece):
        src = w_ref.at[pl.ds(piece * chunk, chunk), :]
        dst = wbuf.at[pl.ds(pl.multiple_of(core * wrows + piece * chunk, chunk), chunk), :]
        recv = w_recv.at[core, piece]
        return (
            pltpu.make_async_copy(src, dst, recv),
            remote(src, dst, w_send.at[0, piece], recv, (2 * z + 1 - y, 2 * x + y)),
            remote(src, dst, w_send.at[1, piece], recv, (me, 2 * x + y)),
        )

    def w_start(piece):
        kept, across, beside = w_part(piece)
        across.start()

        @pl.when(core == y)
        def _():
            kept.start()

        @pl.when(core != y)
        def _():
            beside.start()

    def w_gate(stage):
        for c, plan in enumerate(W_PLAN):
            if plan[stage]:
                @pl.when(core == c)
                def _(plan=plan):
                    for piece in range(sum(plan[:stage]), sum(plan[:stage + 1])):
                        w_start(piece)

    pl.semaphore_wait(barrier, nz + 6)

    by_distance(lambda to: hand_out(to, start, start))
    w_gate(0)

    deep = nz // STEPS
    part = deep * rows
    row_id = lax.broadcasted_iota(jnp.int32, (part, 1), 0)
    row_pos = row_id + y * rows
    for index in range(1, deep):
        row_pos = row_pos + jnp.where(row_id >= index * rows, rows, 0)

    def att_part(c, source, step):
        return att.at[c * nz + source, pl.ds(step * part, part), :]

    def along(to, step, act, act_own=None):
        to_peer(
            to, mine.at[pl.ds(step * part, part), :], att_part(core, z, step),
            z_send.at[to, step], z_recv.at[z, step], act, act_own,
        )

    def forward(source, step):
        ref = att_part(core, source, step)
        return remote(ref, ref, f_send.at[source, step], f_recv.at[source, step], partner)

    def receive(source):
        arrived(docbuf.at[2 * source + y], d_recv.at[source])
        arrived(inbox.at[2 * source + y], i_recv.at[source])
        share(source, start)

    by_distance(receive)
    w_gate(1)

    for step in range(STEPS):
        for source in range(deep * step, deep * (step + 1)):
            arrived(docbuf.at[2 * source + 1 - y], e_recv.at[source])
            arrived(
                inbox.at[2 * source + 1 - y, pl.ds(rows, tall - rows), :], b_recv.at[source]
            )
        seen = range(2 * deep * (step + 1))
        mine[step * part:(step + 1) * part, :] = attention(
            jnp.concatenate(
                [inbox[2 * k + y, :rows, :] for k in range(deep * step, deep * (step + 1))],
                axis=0,
            ),
            jnp.concatenate([inbox[source, rows:2 * rows, :] for source in seen], axis=0),
            jnp.concatenate([inbox[source, 2 * rows:3 * rows, :] for source in seen], axis=0),
            jnp.concatenate(
                [docbuf[source].astype(jnp.float32) for source in seen],
                axis=1,
            ),
            row_pos + 2 * part * step,
        )
        by_distance(lambda to, step=step: along(to, step, start, start), far_first=True)
        w_gate(2 + step)

    slot = 2 * x + core

    def deliver(block, act, act_own=None):
        own = (me == 2 * block + y) & (head == z)
        src = sendbuf.at[pl.ds(block * rows, rows), :]

        if act_own:
            @pl.when(own)
            def _():
                act_own(pltpu.make_async_copy(src, parts.at[slot], p_recv.at[slot]))

        @pl.when(jnp.logical_not(own))
        def _():
            act(remote(
                src, parts.at[slot], p_send.at[block], p_recv.at[slot], (2 * block + y, z)
            ))

    def pass_on(step):
        def one(source):
            arrived(att_part(core, source, step), z_recv.at[source, step])
            forward(source, step).start()

        by_distance(one)

    pass_on(0)

    @pl.when(core != y)
    def _():
        for step in range(1, STEPS):
            pass_on(step)

    for step in range(STEPS):
        if step:
            @pl.when(core == y)
            def _(step=step):
                pass_on(step)

        for source in range(nz):
            arrived(att_part(1 - core, source, step), f_recv.at[source, step])
        if step == 0:
            for index in range(2):
                for piece in range(PIECES):
                    arrived(
                        wbuf.at[pl.ds(index * wrows + piece * chunk, chunk), :],
                        w_recv.at[index, piece],
                    )
        attended = jnp.concatenate(
            [att[index, step * part:(step + 1) * part, :] for index in range(2 * nz)], axis=1
        )
        sendbuf[step * part:(step + 1) * part, :] = jnp.dot(
            attended, wbuf[...], preferred_element_type=jnp.float32
        ).astype(jnp.bfloat16)
        for block in range(deep * step, deep * (step + 1)):
            deliver(block if step == 0 else deep * (2 * step + 1) - 1 - block, start, start)

    res_copy.wait()
    for c in range(2):
        for p in range(2):
            arrived(parts.at[2 * p + c], p_recv.at[2 * p + c])
        cols = slice(c * wcols, (c + 1) * wcols)
        total = parts[c].astype(jnp.float32) + parts[2 + c].astype(jnp.float32)
        out_ref[:, cols] = (resbuf[:, cols].astype(jnp.float32) + total).astype(jnp.bfloat16)

    by_distance(lambda to: hand_out(to, sent))
    for source in range(nz):
        share(source, sent)
    for piece in range(PIECES):
        _, across, beside = w_part(piece)
        across.wait_send()

        @pl.when(core != y)
        def _(beside=beside):
            beside.wait_send()

    for step in range(STEPS):
        by_distance(lambda to, step=step: along(to, step, sent))
        for source in range(nz):
            forward(source, step).wait_send()
    for block in range(nz):
        deliver(block, sent)


def fused(n, query, key_states, value_states, doc_ids, out_weight, residual):
    rows, width = key_states.shape
    wrows, wcols = out_weight.shape
    seq, nz = n * rows, n // 2
    dma = pltpu.SemaphoreType.DMA
    any_ = pl.BlockSpec(memory_space=pl.ANY)
    bf16 = jnp.bfloat16
    return pl.pallas_call(
        functools.partial(fused_kernel, nz),
        out_shape=jax.ShapeDtypeStruct(residual.shape, residual.dtype),
        in_specs=[any_] * 6,
        out_specs=pl.BlockSpec(memory_space=pltpu.VMEM),
        scratch_shapes=[
            pltpu.VMEM((3 * rows, width), bf16),
            pltpu.VMEM((1, rows), jnp.int32),
            pltpu.VMEM((n, 3 * rows, HEAD_DIM), bf16),
            pltpu.VMEM((n, 1, rows), jnp.int32),
            pltpu.VMEM((seq // 2, HEAD_DIM), bf16),
            pltpu.VMEM((n, seq // 2, HEAD_DIM), bf16),
            pltpu.VMEM((2 * wrows, wcols), bf16),
            pltpu.VMEM((seq // 2, wcols), bf16),
            pltpu.VMEM((4, rows, wcols), bf16),
            pltpu.VMEM(residual.shape, bf16),
            dma((4,)),
            dma((nz,)), dma((nz,)),
            dma((nz,)), dma((nz,)),
            dma((nz,)), dma((nz,)),
            dma((nz,)), dma((nz,)),
            dma((nz, STEPS)), dma((nz, STEPS)),
            dma((nz, STEPS)), dma((nz, STEPS)),
            dma((nz,)), dma((4,)),
            dma((2, PIECES)), dma((2, PIECES)), dma,
        ],
        compiler_params=pltpu.CompilerParams(collective_id=0, has_side_effects=True, vmem_limit_bytes=16 << 20),
    )(*[pltpu.with_memory_space_constraint(a, pltpu.HBM) for a in (query, key_states, value_states, doc_ids.reshape(1, rows), out_weight, residual)])


def solution(mesh):
    placed = (
        P("seq", "head"),
        P("seq", "head"),
        P("seq", "head"),
        P("seq"),
        P("head", "seq"),
        P("seq", "head"),
    )
    n, nh = mesh.shape["seq"], mesh.shape["head"]

    def body(query, key_states, value_states, doc_ids, out_weight, residual):
        heads = query.shape[1] // HEAD_DIM
        fits = (
            n == 2 * heads
            and n == 2 * nh
            and nh == 4
            and out_weight.shape[0] % (16 * PIECES) == 0
            and out_weight.shape[1] % 256 == 0
            and query.shape[0] % 16 == 0
            and query.shape[0] <= HEAD_DIM
        )
        run = functools.partial(fused, n) if fits else shards
        return run(query, key_states, value_states, doc_ids, out_weight, residual)

    return jax.shard_map(
        body, mesh=mesh, in_specs=placed, out_specs=P("seq", "head"), check_vma=False
    )
```

```python
import functools

import jax
import jax.numpy as jnp
from jax import lax
from jax.experimental import pallas as pl
from jax.experimental.pallas import tpu as pltpu
from jax.sharding import PartitionSpec as P

HEAD_DIM = 128


masked_score = -1e30


def to_heads(block):
    return block.reshape(block.shape[0], block.shape[1] // HEAD_DIM, HEAD_DIM)


def attend_block(state, queries, query_pos, query_docs, keys, values, key_pos, key_docs):
    run_max, run_sum, run_acc = state
    scores = jnp.einsum(
        "qhd,khd->hqk", queries, keys, preferred_element_type=jnp.float32
    ) * HEAD_DIM ** (-0.5)
    allowed = (key_pos[None, :] <= query_pos[:, None]) & (key_docs[None, :] == query_docs[:, None])
    scores = jnp.where(allowed[None], scores, masked_score)
    new_max = jnp.maximum(run_max, jnp.max(scores, axis=-1))
    weights = jnp.where(allowed[None], jnp.exp(scores - new_max[..., None]), 0.0)
    run_sum = jnp.sum(weights, axis=-1)
    run_acc = jnp.einsum(
        "hqk,khd->hqd", weights.astype(jnp.bfloat16), values, preferred_element_type=jnp.float32
    )
    return (new_max, run_sum, run_acc)


def shards(query, key_states, value_states, doc_ids, out_weight, residual):
    tok_rows = query.shape[0]
    heads = query.shape[1] // HEAD_DIM
    shard_index = lax.axis_index("seq")
    first_pos = shard_index * tok_rows
    groups = [(query, first_pos + jnp.arange(tok_rows, dtype=jnp.int32), doc_ids)]
    prepared = [(to_heads(block), block_pos, block_docs) for block, block_pos, block_docs in groups]
    initial = tuple(
        (
            (
                jnp.full((heads, block_pos.shape[0]), masked_score, jnp.float32),
                jnp.zeros((heads, block_pos.shape[0]), jnp.float32),
                jnp.zeros((heads, block_pos.shape[0], HEAD_DIM), jnp.float32),
            )
            for block, block_pos, block_docs in groups
        )
    )
    first_row = jnp.int32(0)
    keys = lax.all_gather(key_states, "seq", axis=0, tiled=True)
    values = lax.all_gather(value_states, "seq", axis=0, tiled=True)
    key_docs = lax.all_gather(doc_ids, "seq", axis=0, tiled=True)
    key_pos = jnp.arange(keys.shape[0], dtype=jnp.int32)
    key_heads = to_heads(keys)
    value_heads = to_heads(values)
    updated = []
    for member, state in zip(prepared, initial):
        queries, query_pos, query_docs = member

        def advance(inner, queries=queries, query_pos=query_pos, query_docs=query_docs):
            return attend_block(
                inner, queries, query_pos, query_docs, key_heads, value_heads, key_pos, key_docs
            )

        def unchanged(inner):
            return inner

        updated.append(lax.cond(first_row <= jnp.max(query_pos), advance, unchanged, state))
    finals = tuple(updated)
    outputs = []
    for run_max, run_sum, run_acc in finals:
        normed = run_acc / run_sum[..., None]
        outputs.append(
            jnp.transpose(normed, (1, 0, 2))
            .reshape(normed.shape[1], heads * HEAD_DIM)
            .astype(jnp.bfloat16)
        )
    attended = outputs[0]
    mapped = jnp.dot(
        attended,
        lax.all_gather(out_weight, "seq", axis=1, tiled=True),
        preferred_element_type=jnp.float32,
    )
    summed = lax.psum_scatter(mapped, "head", scatter_dimension=1, tiled=True)
    return (residual.astype(jnp.float32) + summed).astype(jnp.bfloat16)


MESH = pl.DeviceIdType.MESH


STEPS = 2
PIECES = 8
W_PLAN = ((3, 2, 3, 0), (2, 0, 2, 4))


def attention(queries, keys, values, doc_row, row_pos):
    rows, keep = queries.shape[0], keys.shape[0]
    scores = lax.dot_general(
        queries, keys, (((1,), (1,)), ((), ())), preferred_element_type=jnp.float32
    ) * HEAD_DIM ** (-0.5)
    col_pos = lax.broadcasted_iota(jnp.int32, (rows, keep), 1)
    docs = jnp.broadcast_to(doc_row, (rows, keep))
    query_docs = jnp.sum(jnp.where(row_pos == col_pos, docs, 0.0), axis=1, keepdims=True)
    allowed = (col_pos <= row_pos) & (docs == query_docs)
    scores = jnp.where(allowed, scores, masked_score)
    row_max = jnp.max(scores, axis=1, keepdims=True)
    weights = jnp.where(allowed, jnp.exp(scores - row_max), 0.0)
    row_sum = jnp.sum(weights, axis=1, keepdims=True)
    product = jnp.dot(weights.astype(jnp.bfloat16), values, preferred_element_type=jnp.float32)
    return (product / row_sum).astype(jnp.bfloat16)


def fused_kernel(
    nz, q_ref, k_ref, v_ref, doc_ref, w_ref, res_ref, out_ref,
    stage, docin, inbox, docbuf, mine, att, wbuf, sendbuf, parts, resbuf,
    in_sem, i_send, i_recv, b_send, b_recv, d_send, d_recv, e_send, e_recv, z_send, z_recv, f_send, f_recv,
    p_send, p_recv, w_send, w_recv, res_sem,
):
    me = lax.axis_index("seq")
    head = lax.axis_index("head")
    rows = k_ref.shape[0]
    z, y = me // 2, me % 2
    x, core = head // 2, head % 2
    wrows = w_ref.shape[0]
    wcols = w_ref.shape[1]

    tall = stage.shape[0]
    chunk = wrows // PIECES

    def peer(to):
        return 2 * to + y, head

    def greet(to):
        pl.semaphore_signal(barrier, inc=1, device_id=to, device_id_type=MESH)

    barrier = pltpu.get_barrier_semaphore()
    for dz in range(1, nz):
        greet(peer(lax.rem(z + dz, nz)))
    for dy in range(2):
        for dh in range(4):
            if dy or dh:
                greet((2 * z + lax.rem(y + dy, 2), lax.rem(head + dh, 4)))

    def arrived(ref, sem):
        pltpu.make_async_copy(ref, ref, sem).wait()

    staged = [
        pltpu.make_async_copy(src, dst, in_sem.at[index])
        for index, (src, dst) in enumerate((
            (doc_ref, docin),
            (q_ref, stage.at[pl.ds(0, rows), :]),
            (k_ref, stage.at[pl.ds(rows, rows), :]),
            (v_ref, stage.at[pl.ds(2 * rows, rows), :]),
        ))
    ]
    for copy in staged:
        copy.start()
    res_copy = pltpu.make_async_copy(res_ref, resbuf, res_sem)
    res_copy.start()

    def remote(src, dst, send, recv, to):
        return pltpu.make_async_remote_copy(
            src_ref=src, dst_ref=dst, send_sem=send, recv_sem=recv,
            device_id=to, device_id_type=MESH,
        )

    def start(copy):
        copy.start()

    def sent(copy):
        copy.wait_send()

    def by_distance(act, far_first=False):
        order = [(0, 0)] + [(far, step) for far in range(1, nz) for step in (far, -far)]
        for far, step in reversed(order) if far_first else order:
            @pl.when((z + step >= 0) & (z + step < nz))
            def _(step=step):
                act(z + step)

    def to_peer(to, src, dst, send, recv, act, act_own):
        own = to == z

        @pl.when(jnp.logical_not(own))
        def _():
            act(remote(src, dst, send, recv, peer(to)))

        if act_own:
            @pl.when(own)
            def _():
                act_own(pltpu.make_async_copy(src, dst, recv))

    partner = (me, 2 * x + 1 - core)

    def hand_out(to, act, act_own=None):
        lanes = pl.ds(pl.multiple_of(to * HEAD_DIM, HEAD_DIM), HEAD_DIM)
        to_peer(to, docin, docbuf.at[me], d_send.at[to], d_recv.at[z], act, act_own)
        to_peer(
            to, stage.at[:, lanes], inbox.at[me], i_send.at[to], i_recv.at[z], act, act_own
        )

    def share(source, act):
        ref = inbox.at[2 * source + y, pl.ds(rows, tall - rows), :]
        numbers = docbuf.at[2 * source + y]
        to = (2 * z + 1 - y, head)
        act(remote(numbers, numbers, e_send.at[source], e_recv.at[source], to))
        act(remote(ref, ref, b_send.at[source], b_recv.at[source], to))

    for copy in staged:
        copy.wait()

    def w_part(piece):
        src = w_ref.at[pl.ds(piece * chunk, chunk), :]
        dst = wbuf.at[pl.ds(pl.multiple_of(core * wrows + piece * chunk, chunk), chunk), :]
        recv = w_recv.at[core, piece]
        return (
            pltpu.make_async_copy(src, dst, recv),
            remote(src, dst, w_send.at[0, piece], recv, (2 * z + 1 - y, 2 * x + y)),
            remote(src, dst, w_send.at[1, piece], recv, (me, 2 * x + y)),
        )

    def w_start(piece):
        kept, across, beside = w_part(piece)
        across.start()

        @pl.when(core == y)
        def _():
            kept.start()

        @pl.when(core != y)
        def _():
            beside.start()

    def w_gate(stage):
        for c, plan in enumerate(W_PLAN):
            if plan[stage]:
                @pl.when(core == c)
                def _(plan=plan):
                    for piece in range(sum(plan[:stage]), sum(plan[:stage + 1])):
                        w_start(piece)

    pl.semaphore_wait(barrier, nz + 6)

    by_distance(lambda to: hand_out(to, start, start))
    w_gate(0)

    deep = nz // STEPS
    part = deep * rows
    row_id = lax.broadcasted_iota(jnp.int32, (part, 1), 0)
    row_pos = row_id + y * rows
    for index in range(1, deep):
        row_pos = row_pos + jnp.where(row_id >= index * rows, rows, 0)

    def att_part(c, source, step):
        return att.at[c * nz + source, pl.ds(step * part, part), :]

    def along(to, step, act, act_own=None):
        to_peer(
            to, mine.at[pl.ds(step * part, part), :], att_part(core, z, step),
            z_send.at[to, step], z_recv.at[z, step], act, act_own,
        )

    def forward(source, step):
        ref = att_part(core, source, step)
        return remote(ref, ref, f_send.at[source, step], f_recv.at[source, step], partner)

    def receive(source):
        arrived(docbuf.at[2 * source + y], d_recv.at[source])
        arrived(inbox.at[2 * source + y], i_recv.at[source])
        share(source, start)

    by_distance(receive)
    w_gate(1)

    for step in range(STEPS):
        for source in range(deep * step, deep * (step + 1)):
            arrived(docbuf.at[2 * source + 1 - y], e_recv.at[source])
            arrived(
                inbox.at[2 * source + 1 - y, pl.ds(rows, tall - rows), :], b_recv.at[source]
            )
        seen = range(2 * deep * (step + 1))
        mine[step * part:(step + 1) * part, :] = attention(
            jnp.concatenate(
                [inbox[2 * k + y, :rows, :] for k in range(deep * step, deep * (step + 1))],
                axis=0,
            ),
            jnp.concatenate([inbox[source, rows:2 * rows, :] for source in seen], axis=0),
            jnp.concatenate([inbox[source, 2 * rows:3 * rows, :] for source in seen], axis=0),
            jnp.concatenate(
                [docbuf[source].astype(jnp.float32) for source in seen],
                axis=1,
            ),
            row_pos + 2 * part * step,
        )
        by_distance(lambda to, step=step: along(to, step, start, start), far_first=True)
        w_gate(2 + step)

    slot = 2 * x + core

    def deliver(block, act, act_own=None):
        own = (me == 2 * block + y) & (head == z)
        src = sendbuf.at[pl.ds(block * rows, rows), :]

        if act_own:
            @pl.when(own)
            def _():
                act_own(pltpu.make_async_copy(src, parts.at[slot], p_recv.at[slot]))

        @pl.when(jnp.logical_not(own))
        def _():
            act(remote(
                src, parts.at[slot], p_send.at[block], p_recv.at[slot], (2 * block + y, z)
            ))

    def pass_on(step):
        def one(source):
            arrived(att_part(core, source, step), z_recv.at[source, step])
            forward(source, step).start()

        by_distance(one)

    pass_on(0)

    @pl.when(core != y)
    def _():
        for step in range(1, STEPS):
            pass_on(step)

    for step in range(STEPS):
        if step:
            @pl.when(core == y)
            def _(step=step):
                pass_on(step)

        for source in range(nz):
            arrived(att_part(1 - core, source, step), f_recv.at[source, step])
        if step == 0:
            for index in range(2):
                for piece in range(PIECES):
                    arrived(
                        wbuf.at[pl.ds(index * wrows + piece * chunk, chunk), :],
                        w_recv.at[index, piece],
                    )
        attended = jnp.concatenate(
            [att[index, step * part:(step + 1) * part, :] for index in range(2 * nz)], axis=1
        )
        sendbuf[step * part:(step + 1) * part, :] = jnp.dot(
            attended, wbuf[...], preferred_element_type=jnp.float32
        ).astype(jnp.bfloat16)
        for block in range(deep * step, deep * (step + 1)):
            deliver(block, start, start)

    res_copy.wait()
    for c in range(2):
        for p in range(2):
            arrived(parts.at[2 * p + c], p_recv.at[2 * p + c])
        cols = slice(c * wcols, (c + 1) * wcols)
        total = parts[c].astype(jnp.float32) + parts[2 + c].astype(jnp.float32)
        out_ref[:, cols] = (resbuf[:, cols].astype(jnp.float32) + total).astype(jnp.bfloat16)

    by_distance(lambda to: hand_out(to, sent))
    for source in range(nz):
        share(source, sent)
    for piece in range(PIECES):
        _, across, beside = w_part(piece)
        across.wait_send()

        @pl.when(core != y)
        def _(beside=beside):
            beside.wait_send()

    for step in range(STEPS):
        by_distance(lambda to, step=step: along(to, step, sent))
        for source in range(nz):
            forward(source, step).wait_send()
    for block in range(nz):
        deliver(block, sent)


def fused(n, query, key_states, value_states, doc_ids, out_weight, residual):
    rows, width = key_states.shape
    wrows, wcols = out_weight.shape
    seq, nz = n * rows, n // 2
    dma = pltpu.SemaphoreType.DMA
    any_ = pl.BlockSpec(memory_space=pl.ANY)
    bf16 = jnp.bfloat16
    return pl.pallas_call(
        functools.partial(fused_kernel, nz),
        out_shape=jax.ShapeDtypeStruct(residual.shape, residual.dtype),
        in_specs=[any_] * 6,
        out_specs=pl.BlockSpec(memory_space=pltpu.VMEM),
        scratch_shapes=[
            pltpu.VMEM((3 * rows, width), bf16),
            pltpu.VMEM((1, rows), jnp.int32),
            pltpu.VMEM((n, 3 * rows, HEAD_DIM), bf16),
            pltpu.VMEM((n, 1, rows), jnp.int32),
            pltpu.VMEM((seq // 2, HEAD_DIM), bf16),
            pltpu.VMEM((n, seq // 2, HEAD_DIM), bf16),
            pltpu.VMEM((2 * wrows, wcols), bf16),
            pltpu.VMEM((seq // 2, wcols), bf16),
            pltpu.VMEM((4, rows, wcols), bf16),
            pltpu.VMEM(residual.shape, bf16),
            dma((4,)),
            dma((nz,)), dma((nz,)),
            dma((nz,)), dma((nz,)),
            dma((nz,)), dma((nz,)),
            dma((nz,)), dma((nz,)),
            dma((nz, STEPS)), dma((nz, STEPS)),
            dma((nz, STEPS)), dma((nz, STEPS)),
            dma((nz,)), dma((4,)),
            dma((2, PIECES)), dma((2, PIECES)), dma,
        ],
        compiler_params=pltpu.CompilerParams(collective_id=0, has_side_effects=True, vmem_limit_bytes=16 << 20),
    )(*[pltpu.with_memory_space_constraint(a, pltpu.HBM) for a in (query, key_states, value_states, doc_ids.reshape(1, rows), out_weight, residual)])


def solution(mesh):
    placed = (
        P("seq", "head"),
        P("seq", "head"),
        P("seq", "head"),
        P("seq"),
        P("head", "seq"),
        P("seq", "head"),
    )
    n, nh = mesh.shape["seq"], mesh.shape["head"]

    def body(query, key_states, value_states, doc_ids, out_weight, residual):
        heads = query.shape[1] // HEAD_DIM
        fits = (
            n == 2 * heads
            and n == 2 * nh
            and nh == 4
            and out_weight.shape[0] % (16 * PIECES) == 0
            and out_weight.shape[1] % 256 == 0
            and query.shape[0] % 16 == 0
            and query.shape[0] <= HEAD_DIM
        )
        run = functools.partial(fused, n) if fits else shards
        return run(query, key_states, value_states, doc_ids, out_weight, residual)

    return jax.shard_map(
        body, mesh=mesh, in_specs=placed, out_specs=P("seq", "head"), check_vma=False
    )
```
